512 devices in a mesh: groups: 2 (over y), row: 32 (over z), col: 4 (over x), sub: 2 (over core).
Axes of the slice: x: 4, y: 2, z: 32, core: 2. Of those that a mesh axis runs over, the one named last changes fastest.
The devices are a block of a 4x16x32 slice.
Arguments:
- matrix: float32 [16384, 8192], P(('groups', 'row'), ('col', 'sub')), parts along dimension 0, may hold values from -60 to 60
- basis_vectors: float32 [16384, 1024], P(('groups', 'row'), ('col', 'sub')), parts along dimension 0, may hold values from -0.0625 to 0.0625
- split_size: int32 [2], P('groups'), parts along dimension 0, may hold values from 256 to 767
Outputs:
- children: float32 [2, 2048, 1024], P('sub', ('groups', 'row'), 'col'), parts along dimension 1
The draws below stay inside these ranges and needn't reach their ends.
There are 2 independent parts, one for each index of `groups`. The reference program is written for one: setup_inputs(seed, part) draws one part's arguments, and reference() takes and returns one part's arrays. A program takes and returns all parts, laid end to end along the dimension named above; each array names one. Nothing has to cross between parts.
Inputs may be any that keep to these rules, and one draw needn't show every extreme that they name: The second subspace has 1024 minus split_size vectors.
All inputs are finite; a program needn't handle non-finite values.
Results may differ from the reference program's by a relative error of at most 0.00011.
Values sent between devices are 32-bit elements; how exact they have to be, the bound alone decides.
No kernel may reach another device: no remote copies, remote signals or barrier semaphores. Data moves between devices by JAX's collectives and lax.ppermute only.
A program may use at most 64 MiB of HBM per device.

```python
import jax
import jax.numpy as jnp
from jax import lax

N = 8192
K = 1024


def draw_matrix(key, part):
    noise = jax.random.normal(key, (N, N), jnp.float32)
    symmetric = (noise + noise.T) * 0.5 ** 0.5
    return symmetric


def level_of(stream_key, dims, split, least, top_value):
    loudness = 1.0
    for position, parts in split:
        steps = jax.random.uniform(jax.random.fold_in(jax.random.fold_in(stream_key, 6), position), (parts,), jnp.float32, least / len(split), top_value / len(split))
        loudness = loudness * jnp.repeat(jnp.exp(steps), dims[position] // parts).reshape((-1,) + (1,) * (len(dims) - 1 - position))
    return loudness


def gaussian(own_key, shape, spread, most, pieces=(), kind=jnp.bfloat16):
    result = jax.random.normal(own_key, shape, jnp.float32) * spread
    if len(pieces) > 0:
        result = level_of(own_key, shape, pieces, -0.22, 0.18) * result
    return jnp.clip(result, min=-most, max=most).astype(kind)


def setup_inputs(seed: int = 0, part: int = 0) -> dict:
    splits = jax.random.split(jax.random.key(seed), 4)
    part_keys = jax.random.split(jax.random.fold_in(splits[3], part), 4)
    return {
        "matrix": draw_matrix(jax.random.fold_in(jax.random.fold_in(splits[3], part), 71), part),
        "basis_vectors": gaussian(part_keys[1], (N, K), N ** -0.5, 0.0625, ((0, 32), (1, 8)), jnp.float32),
        "split_size": jax.random.randint(part_keys[2], (1,), K // 4, 3 * K // 4).astype(jnp.int32),
    }


def reference(matrix, basis_vectors, split_size):
    image = jnp.dot(matrix, basis_vectors, precision=lax.Precision.HIGHEST, preferred_element_type=jnp.float32)
    projected = jnp.dot(basis_vectors.T, image, precision=lax.Precision.HIGHEST, preferred_element_type=jnp.float32)
    positions = jnp.arange(K, dtype=jnp.int32)
    in_first = positions < split_size[0]
    in_second = jnp.logical_not(in_first)
    mask_one = in_first[:, None] & in_first[None, :]
    mask_two = in_second[:, None] & in_second[None, :]
    nothing = jnp.zeros((), jnp.float32)
    return jnp.stack([jnp.where(mask_one, projected, nothing), jnp.where(mask_two, projected, nothing)])
```

```python
import jax
import jax.numpy as jnp
from jax import lax
from jax.sharding import PartitionSpec as P

PRECISION = lax.Precision.HIGHEST
NEAR = 4


def shifted(array, axis, step):
    size = lax.axis_size(axis)
    return lax.ppermute(array, axis, [(i, (i + step) % size) for i in range(size)])


def swapped(array, axis):
    size = lax.axis_size(axis)
    return lax.ppermute(array, axis, [(i, i ^ 1) for i in range(size)])


def product(left, right, contract):
    return lax.dot_general(
        left, right, (contract, ((), ())), precision=PRECISION, preferred_element_type=jnp.float32
    )


def all_columns(basis):
    half = basis.shape[0] // 2
    parts = [lax.all_gather(basis[i * half : (i + 1) * half], ("col", "sub"), axis=0) for i in range(2)]
    return parts


def shards(matrix, basis_vectors, split_size):
    rows_here, width = matrix.shape
    n_row = lax.axis_size("row")
    n_col = lax.axis_size("col")
    row = lax.axis_index("row")
    col = lax.axis_index("col")
    sub = lax.axis_index("sub")
    parity = row % 2

    every_other = [[first + 2 * i for i in range(n_row // 2)] for first in range(2)]
    strip = lax.all_gather(
        basis_vectors, "row", axis=0, tiled=True, axis_index_groups=every_other
    )

    blocks = matrix.reshape(rows_here, width // (2 * rows_here), 2, rows_here)
    keep = jnp.where(parity == 0, blocks[:, :, 0], blocks[:, :, 1]).reshape(rows_here, width // 2)
    give = jnp.where(parity == 0, blocks[:, :, 1], blocks[:, :, 0]).reshape(rows_here, width // 2)
    own = jnp.concatenate([keep, swapped(give, "row")], axis=0)

    before = shifted(own, "col", 1)
    after = shifted(own, "col", -1)
    half = own.shape[0] // 2
    across = jnp.concatenate(
        [shifted(before[:half], "col", 1), shifted(after[half:], "col", -1)], axis=0
    )
    pieces = {0: own, 1: before, 2: across, 3: after}

    mate = swapped(basis_vectors, "row")
    pair_basis = jnp.concatenate(all_columns(basis_vectors) + all_columns(mate), axis=1)

    span = own.shape[1]
    image = None
    for distance, piece in pieces.items():
        source = (col - distance) % n_col
        other = swapped(piece, "sub")
        for core, operand in ((sub, piece), (1 - sub, other)):
            rows = lax.dynamic_slice_in_dim(strip, (source * 2 + core) * span, span, 0)
            part = product(operand, rows, ((1,), (0,)))
            image = part if image is None else image + part

    partial = product(pair_basis, image, ((1,), (0,)))
    total = partial.shape[0] * partial.shape[1]
    share = total // n_row
    far = n_row // NEAR
    partial = partial.reshape(far, NEAR, share, -1).swapaxes(0, 1)
    near_groups = [[NEAR * g + q for q in range(NEAR)] for g in range(far)]
    far_groups = [[NEAR * g + q for g in range(far)] for q in range(NEAR)]
    partial = lax.all_to_all(
        partial, "row", 0, 0, tiled=True, axis_index_groups=near_groups
    ).sum(0)
    proj_block = lax.all_to_all(
        partial, "row", 0, 0, tiled=True, axis_index_groups=far_groups
    ).sum(0)

    child_block = lax.all_gather(proj_block, "sub", axis=1, tiled=True)
    row_ids = jnp.arange(child_block.shape[0], dtype=jnp.int32) + row * child_block.shape[0]
    col_ids = jnp.arange(child_block.shape[1], dtype=jnp.int32) + col * child_block.shape[1]
    leading = split_size[0]
    row_first = row_ids < leading
    col_first = col_ids < leading
    mask_one = row_first[:, None] & col_first[None, :]
    mask_two = jnp.logical_not(row_first)[:, None] & jnp.logical_not(col_first)[None, :]
    selected = jnp.where(sub == 0, mask_one, mask_two)
    return jnp.where(selected, child_block, jnp.zeros((), jnp.float32))[None]


def solution(mesh):
    placed = (
        P(("groups", "row"), ("col", "sub")),
        P(("groups", "row"), ("col", "sub")),
        P("groups"),
    )
    return jax.shard_map(
        shards,
        mesh=mesh,
        in_specs=placed,
        out_specs=P("sub", ("groups", "row"), "col"),
        check_vma=False,
    )
```

```python
import functools

import jax
import jax.numpy as jnp
from jax import lax
from jax.experimental import pallas as pl
from jax.experimental.pallas import tpu as pltpu
from jax.sharding import PartitionSpec as P


NEAR = 4
STEPS = 4


def shifted(array, axis, step):
    size = lax.axis_size(axis)
    return lax.ppermute(array, axis, [(i, (i + step) % size) for i in range(size)])


def swapped(array, axis):
    size = lax.axis_size(axis)
    return lax.ppermute(array, axis, [(i, i ^ 1) for i in range(size)])


def halves(value):
    high = value.astype(jnp.bfloat16)
    low = (value - high.astype(jnp.float32)).astype(jnp.bfloat16)
    return high, low


def dot(left, right):
    return jnp.dot(left, right, preferred_element_type=jnp.float32)


def project_kernel(starts, strip, basis_t, *refs, n_whole, near):
    whole, (top, bottom), (top_o, bottom_o) = refs[:n_whole], refs[n_whole : n_whole + 2], refs[n_whole + 2 : n_whole + 4]
    out, strip2, image2 = refs[n_whole + 4 :]
    step = pl.program_id(0)
    steps = pl.num_programs(0)
    wide = strip.shape[1]
    tile, span = whole[0].shape

    @pl.when(step == 0)
    def _():
        high, low = halves(strip[...])
        strip2[:, :wide] = high
        strip2[:, wide:] = low

    first = step < steps // 2
    pieces = [ref[...] for ref in whole]
    pieces.append(jnp.where(first, top[...], bottom[...]))
    pieces.append(jnp.where(first, top_o[...], bottom_o[...]))
    both = jnp.zeros((tile, 2 * wide), jnp.float32)
    rest = jnp.zeros((tile, wide), jnp.float32)
    for n, piece in enumerate(pieces):
        high, low = halves(piece)
        start = pl.multiple_of(starts[n] * span, span)
        both += dot(high, strip2[pl.ds(start, span), :])
        rest += dot(low, strip2[pl.ds(start, span), :wide])
    high, low = halves(both[:, :wide] + (both[:, wide:] + rest))
    image2[pl.ds(pl.multiple_of(step * tile, tile), tile), :wide] = high
    image2[pl.ds(pl.multiple_of(step * tile, tile), tile), wide:] = low

    @pl.when(step == steps - 1)
    def _():
        high, low = halves(basis_t[...])
        both = dot(high, image2[...])
        proj = both[:, :wide] + (both[:, wide:] + dot(low, image2[:, :wide]))
        far, share = out.shape[1], out.shape[2]
        for f in range(far):
            for q in range(near):
                begin = (f * near + q) * share
                out[q, f] = proj[begin : begin + share]


def projected(starts, strip, basis_t, whole, across, across_other, share):
    rows, span = whole[0].shape
    tile = rows // STEPS
    total, wide = basis_t.shape[0], strip.shape[1]
    last = STEPS // 2 - 1
    far = total // share // NEAR
    tiled = pl.BlockSpec((tile, span), lambda i, s: (i, 0))
    low = pl.BlockSpec((tile, span), lambda i, s: (jnp.minimum(i, last), 0))
    high = pl.BlockSpec((tile, span), lambda i, s: (jnp.maximum(i - last - 1, 0), 0))
    fixed = lambda shape: pl.BlockSpec(shape, lambda i, s: (0,) * len(shape))
    out_shape = (NEAR, far, share, wide)
    return pl.pallas_call(
        functools.partial(project_kernel, n_whole=len(whole), near=NEAR),
        grid_spec=pltpu.PrefetchScalarGridSpec(
            num_scalar_prefetch=1,
            grid=(STEPS,),
            in_specs=[fixed(strip.shape), fixed(basis_t.shape)]
            + [tiled] * len(whole)
            + [low, high, low, high],
            out_specs=fixed(out_shape),
            scratch_shapes=[
                pltpu.VMEM((strip.shape[0], 2 * wide), jnp.bfloat16),
                pltpu.VMEM((rows, 2 * wide), jnp.bfloat16),
            ],
        ),
        out_shape=jax.ShapeDtypeStruct(out_shape, jnp.float32),
        compiler_params=pltpu.CompilerParams(
            dimension_semantics=("arbitrary",), vmem_limit_bytes=40 * 2**20
        ),
        cost_estimate=pl.CostEstimate(
            flops=3 * 2 * rows * wide * (strip.shape[0] + total),
            bytes_accessed=4 * (strip.size + basis_t.size + rows * strip.shape[0]),
            transcendentals=0,
        ),
        name="project",
    )(starts, strip, basis_t, *whole, *across, *across_other)


def split_projection(matrix, basis_vectors, split_size):
    block, width = matrix.shape
    n_row = lax.axis_size("row")
    n_col = lax.axis_size("col")
    row = lax.axis_index("row")
    col = lax.axis_index("col")
    sub = lax.axis_index("sub")
    even = row % 2 == 0

    every_other = [[first + 2 * i for i in range(n_row // 2)] for first in range(2)]
    strip = lax.all_gather(
        basis_vectors, "row", axis=0, tiled=True, axis_index_groups=every_other
    )

    mate = swapped(basis_vectors, "row")
    pair_t = jnp.concatenate([basis_vectors, mate], axis=0).T
    pair_t = jnp.broadcast_to(pair_t[None], (n_col * lax.axis_size("sub"), *pair_t.shape))

    blocks = [matrix[:, i * block : (i + 1) * block] for i in range(width // block)]
    keep = jnp.concatenate(
        [jnp.where(even, a, b) for a, b in zip(blocks[::2], blocks[1::2])], axis=1
    )
    give = jnp.concatenate(
        [jnp.where(even, b, a) for a, b in zip(blocks[::2], blocks[1::2])], axis=1
    )
    basis_t = lax.all_to_all(pair_t, ("col", "sub"), 0, 0, tiled=True).reshape(-1, 2 * block)
    received = swapped(give, "row")
    own = jnp.concatenate([keep, received], axis=0)

    before = shifted(own, "col", 1)
    after = shifted(own, "col", -1)
    across = (shifted(before[:block], "col", 1), shifted(after[block:], "col", -1))
    mine = [own, before, after]
    theirs = [swapped(piece, "sub") for piece in mine]
    across_other = tuple(swapped(piece, "sub") for piece in across)

    sources = [col, (col - 1) % n_col, (col + 1) % n_col]
    opposite = (col + 2) % n_col
    starts = jnp.stack(
        [2 * s + sub for s in sources]
        + [2 * s + 1 - sub for s in sources]
        + [2 * opposite + sub, 2 * opposite + 1 - sub]
    ).astype(jnp.int32)
    share = basis_t.shape[0] // n_row
    partial = projected(starts, strip, basis_t, mine + theirs, across, across_other, share)

    far = n_row // NEAR
    near_groups = [[NEAR * g + q for q in range(NEAR)] for g in range(far)]
    far_groups = [[NEAR * g + q for g in range(far)] for q in range(NEAR)]
    partial = lax.all_to_all(
        partial, "row", 0, 0, tiled=True, axis_index_groups=near_groups
    ).sum(0)
    proj_block = lax.all_to_all(
        partial, "row", 0, 0, tiled=True, axis_index_groups=far_groups
    ).sum(0)

    child_block = lax.all_gather(proj_block, "sub", axis=1, tiled=True)
    row_ids = jnp.arange(child_block.shape[0], dtype=jnp.int32) + row * child_block.shape[0]
    col_ids = jnp.arange(child_block.shape[1], dtype=jnp.int32) + col * child_block.shape[1]
    leading = split_size[0]
    row_first = row_ids < leading
    col_first = col_ids < leading
    mask_one = row_first[:, None] & col_first[None, :]
    mask_two = jnp.logical_not(row_first)[:, None] & jnp.logical_not(col_first)[None, :]
    selected = jnp.where(sub == 0, mask_one, mask_two)
    return jnp.where(selected, child_block, jnp.zeros((), jnp.float32))[None]


def solution(mesh):
    placed = (
        P(("groups", "row"), ("col", "sub")),
        P(("groups", "row"), ("col", "sub")),
        P("groups"),
    )
    return jax.shard_map(
        split_projection,
        mesh=mesh,
        in_specs=placed,
        out_specs=P("sub", ("groups", "row"), "col"),
        check_vma=False,
    )
```

```python
import functools

import jax
import jax.numpy as jnp
from jax import lax
from jax.experimental import pallas as pl
from jax.experimental.pallas import tpu as pltpu
from jax.sharding import PartitionSpec as P


NEAR = 4
TILE = 256


def shifted(array, axis, step):
    size = lax.axis_size(axis)
    return lax.ppermute(array, axis, [(i, (i + step) % size) for i in range(size)])


def swapped(array, axis):
    size = lax.axis_size(axis)
    return lax.ppermute(array, axis, [(i, i ^ 1) for i in range(size)])


def halves(value):
    high = value.astype(jnp.bfloat16)
    low = (value - high.astype(jnp.float32)).astype(jnp.bfloat16)
    return high, low


def dot(left, right):
    return jnp.dot(left, right, preferred_element_type=jnp.float32)


def project_kernel(starts, strip, basis_t, *refs, n_whole):
    parts = [(ref,) for ref in refs[:n_whole]]
    parts += [refs[n_whole : n_whole + 2], refs[n_whole + 2 : n_whole + 4]]
    out, chunks, tiles, arrived, landed, image = refs[n_whole + 4 :]
    wide = strip.shape[1]
    span = chunks.shape[1]
    per_piece = tiles.shape[1] // TILE

    def chunk_copy(n):
        rows = pl.ds(pl.multiple_of(starts[n] * span, span), span)
        return pltpu.make_async_copy(strip.at[rows], chunks.at[n], arrived.at[n])

    def tile_copy(n, t):
        ref, row = parts[n][t * len(parts[n]) // per_piece], t * TILE
        source = ref.at[pl.ds(row % ref.shape[0], TILE)]
        return pltpu.make_async_copy(source, tiles.at[n, pl.ds(row, TILE)], landed.at[n, t])

    for n in range(len(parts)):
        chunk_copy(n).start()
        for t in range(per_piece):
            tile_copy(n, t).start()
    for n in range(len(parts)):
        chunk_copy(n).wait()
        high, low = halves(chunks[n])
        right = jnp.concatenate([high, low], axis=1)
        for t in range(per_piece):
            tile_copy(n, t).wait()
            here = slice(t * TILE, (t + 1) * TILE)
            left_high, left_low = halves(tiles[n, here])
            both = dot(left_high, right)
            value = both[:, :wide] + (both[:, wide:] + dot(left_low, high))
            if n == 0:
                image[here, :] = value
            else:
                image[here, :] += value

    high, low = halves(image[...])
    right = jnp.concatenate([high, low], axis=1)
    near, far, share = out.shape[:3]
    for f in range(far):
        rows = near * share
        left_high, left_low = halves(basis_t[f * rows : (f + 1) * rows, :])
        both = dot(left_high, right)
        proj = both[:, :wide] + (both[:, wide:] + dot(left_low, high))
        for q in range(near):
            out[q, f] = proj[q * share : (q + 1) * share]


def projected(starts, strip, basis_t, whole, across, across_other, share):
    rows, span = whole[0].shape
    total, wide = basis_t.shape[0], strip.shape[1]
    n_pieces = len(whole) + 2
    out_shape = (NEAR, total // share // NEAR, share, wide)
    vmem = pl.BlockSpec(memory_space=pltpu.VMEM)
    anywhere = pl.BlockSpec(memory_space=pl.ANY)
    strip = pltpu.with_memory_space_constraint(strip, pltpu.HBM)
    return pl.pallas_call(
        functools.partial(project_kernel, n_whole=len(whole)),
        in_specs=[pl.BlockSpec(memory_space=pltpu.SMEM), anywhere, vmem]
        + [anywhere] * (len(whole) + 4),
        out_specs=vmem,
        scratch_shapes=[
            pltpu.VMEM((n_pieces, span, wide), jnp.float32),
            pltpu.VMEM((n_pieces, rows, span), jnp.float32),
            pltpu.SemaphoreType.DMA((n_pieces,)),
            pltpu.SemaphoreType.DMA((n_pieces, rows // TILE)),
            pltpu.VMEM((rows, wide), jnp.float32),
        ],
        out_shape=jax.ShapeDtypeStruct(out_shape, jnp.float32),
        compiler_params=pltpu.CompilerParams(vmem_limit_bytes=32 * 2**20),
        cost_estimate=pl.CostEstimate(
            flops=3 * 2 * rows * wide * (strip.shape[0] + total),
            bytes_accessed=4 * (strip.size + basis_t.size + rows * strip.shape[0]),
            transcendentals=0,
        ),
        name="project",
    )(starts, strip, basis_t, *whole, *across, *across_other)


def split_projection(matrix, basis_vectors, split_size):
    block, width = matrix.shape
    n_row = lax.axis_size("row")
    n_col = lax.axis_size("col")
    row = lax.axis_index("row")
    col = lax.axis_index("col")
    sub = lax.axis_index("sub")
    even = row % 2 == 0

    every_other = [[first + 2 * i for i in range(n_row // 2)] for first in range(2)]
    strip = lax.all_gather(
        basis_vectors, "row", axis=0, tiled=True, axis_index_groups=every_other
    )

    mate = swapped(basis_vectors, "row")
    pair_t = jnp.concatenate([basis_vectors, mate], axis=0).T
    pair_t = jnp.broadcast_to(pair_t[None], (n_col * lax.axis_size("sub"), *pair_t.shape))

    blocks = [matrix[:, i * block : (i + 1) * block] for i in range(width // block)]
    keep = jnp.concatenate(
        [jnp.where(even, a, b) for a, b in zip(blocks[::2], blocks[1::2])], axis=1
    )
    give = jnp.concatenate(
        [jnp.where(even, b, a) for a, b in zip(blocks[::2], blocks[1::2])], axis=1
    )
    basis_t = lax.all_to_all(pair_t, ("col", "sub"), 0, 0, tiled=True).reshape(-1, 2 * block)
    received = swapped(give, "row")
    own = jnp.concatenate([keep, received], axis=0)

    before = shifted(own, "col", 1)
    after = shifted(own, "col", -1)
    across = (shifted(before[:block], "col", 1), shifted(after[block:], "col", -1))
    mine = [own, before, after]
    theirs = [swapped(piece, "sub") for piece in mine]
    across_other = tuple(swapped(piece, "sub") for piece in across)

    sources = [col, (col - 1) % n_col, (col + 1) % n_col]
    opposite = (col + 2) % n_col
    starts = jnp.stack(
        [2 * s + sub for s in sources]
        + [2 * s + 1 - sub for s in sources]
        + [2 * opposite + sub, 2 * opposite + 1 - sub]
    ).astype(jnp.int32)
    share = basis_t.shape[0] // n_row
    partial = projected(starts, strip, basis_t, mine + theirs, across, across_other, share)

    far = n_row // NEAR
    near_groups = [[NEAR * g + q for q in range(NEAR)] for g in range(far)]
    far_groups = [[NEAR * g + q for g in range(far)] for q in range(NEAR)]
    partial = lax.all_to_all(
        partial, "row", 0, 0, tiled=True, axis_index_groups=near_groups
    ).sum(0)
    proj_block = lax.all_to_all(
        partial, "row", 0, 0, tiled=True, axis_index_groups=far_groups
    ).sum(0)

    child_block = lax.all_gather(proj_block, "sub", axis=1, tiled=True)
    row_ids = jnp.arange(child_block.shape[0], dtype=jnp.int32) + row * child_block.shape[0]
    col_ids = jnp.arange(child_block.shape[1], dtype=jnp.int32) + col * child_block.shape[1]
    leading = split_size[0]
    row_first = row_ids < leading
    col_first = col_ids < leading
    mask_one = row_first[:, None] & col_first[None, :]
    mask_two = jnp.logical_not(row_first)[:, None] & jnp.logical_not(col_first)[None, :]
    selected = jnp.where(sub == 0, mask_one, mask_two)
    return jnp.where(selected, child_block, jnp.zeros((), jnp.float32))[None]


def solution(mesh):
    placed = (
        P(("groups", "row"), ("col", "sub")),
        P(("groups", "row"), ("col", "sub")),
        P("groups"),
    )
    return jax.shard_map(
        split_projection,
        mesh=mesh,
        in_specs=placed,
        out_specs=P("sub", ("groups", "row"), "col"),
        check_vma=False,
    )
```

```python
import jax
import jax.numpy as jnp
from jax import lax
from jax.experimental import pallas as pl
from jax.experimental.pallas import tpu as pltpu
from jax.sharding import PartitionSpec as P


NEAR = 4
TILE = 256
AHEAD = 3


def shifted(array, axis, step):
    size = lax.axis_size(axis)
    return lax.ppermute(array, axis, [(i, (i + step) % size) for i in range(size)])


def swapped(array, axis):
    size = lax.axis_size(axis)
    return lax.ppermute(array, axis, [(i, i ^ 1) for i in range(size)])


def halves(value):
    high = value.astype(jnp.bfloat16)
    low = (value - high.astype(jnp.float32)).astype(jnp.bfloat16)
    return high, low


def dot(left, right):
    return jnp.dot(left, right, preferred_element_type=jnp.float32)


def project_kernel(starts, strip, basis_t, *refs):
    *pieces, out, chunks, tiles, arrived, landed, image = refs
    wide = strip.shape[1]
    span = chunks.shape[1]
    per_piece = tiles.shape[1] // TILE

    def chunk_copy(n):
        rows = pl.ds(pl.multiple_of(starts[n] * span, span), span)
        return pltpu.make_async_copy(strip.at[rows], chunks.at[n], arrived.at[n])

    def tile_copy(n, t):
        rows = pl.ds(t * TILE, TILE)
        return pltpu.make_async_copy(pieces[n].at[rows], tiles.at[n, rows], landed.at[n, t])

    def begin(n):
        chunk_copy(n).start()
        for t in range(per_piece):
            tile_copy(n, t).start()

    for n in range(AHEAD):
        begin(n)
    for n in range(len(pieces)):
        if n + AHEAD < len(pieces):
            begin(n + AHEAD)
        chunk_copy(n).wait()
        high, low = halves(chunks[n])
        right = jnp.concatenate([high, low], axis=1)
        for t in range(per_piece):
            tile_copy(n, t).wait()
            here = slice(t * TILE, (t + 1) * TILE)
            left_high, left_low = halves(tiles[n, here])
            both = dot(left_high, right)
            value = both[:, :wide] + (both[:, wide:] + dot(left_low, high))
            if n == 0:
                image[here, :] = value
            else:
                image[here, :] += value

    high, low = halves(image[...])
    right = jnp.concatenate([high, low], axis=1)
    near, far, share = out.shape[:3]
    for f in range(far):
        rows = near * share
        left_high, left_low = halves(basis_t[f * rows : (f + 1) * rows, :])
        both = dot(left_high, right)
        proj = both[:, :wide] + (both[:, wide:] + dot(left_low, high))
        for q in range(near):
            out[q, f] = proj[q * share : (q + 1) * share]


def projected(starts, strip, basis_t, pieces, share):
    rows, span = pieces[0].shape
    total, wide = basis_t.shape[0], strip.shape[1]
    n_pieces = len(pieces)
    out_shape = (NEAR, total // share // NEAR, share, wide)
    vmem = pl.BlockSpec(memory_space=pltpu.VMEM)
    anywhere = pl.BlockSpec(memory_space=pl.ANY)
    strip = pltpu.with_memory_space_constraint(strip, pltpu.HBM)
    return pl.pallas_call(
        project_kernel,
        in_specs=[pl.BlockSpec(memory_space=pltpu.SMEM), anywhere, vmem]
        + [anywhere] * n_pieces,
        out_specs=vmem,
        scratch_shapes=[
            pltpu.VMEM((n_pieces, span, wide), jnp.float32),
            pltpu.VMEM((n_pieces, rows, span), jnp.float32),
            pltpu.SemaphoreType.DMA((n_pieces,)),
            pltpu.SemaphoreType.DMA((n_pieces, rows // TILE)),
            pltpu.VMEM((rows, wide), jnp.float32),
        ],
        out_shape=jax.ShapeDtypeStruct(out_shape, jnp.float32),
        compiler_params=pltpu.CompilerParams(vmem_limit_bytes=32 * 2**20),
        cost_estimate=pl.CostEstimate(
            flops=3 * 2 * rows * wide * (strip.shape[0] + total),
            bytes_accessed=4 * (strip.size + basis_t.size + rows * strip.shape[0]),
            transcendentals=0,
        ),
        name="project",
    )(starts, strip, basis_t, *pieces)


def kept(leading, row, col, sub, height, width):
    row_ids = jnp.arange(height, dtype=jnp.int32) + row * height
    col_ids = jnp.arange(width, dtype=jnp.int32) + col * width
    row_first = row_ids < leading
    col_first = col_ids < leading
    mask_one = row_first[:, None] & col_first[None, :]
    mask_two = jnp.logical_not(row_first)[:, None] & jnp.logical_not(col_first)[None, :]
    return jnp.where(sub == 0, mask_one, mask_two)


def split_projection(matrix, basis_vectors, split_size):
    block, width = matrix.shape
    n_row = lax.axis_size("row")
    n_col = lax.axis_size("col")
    row = lax.axis_index("row")
    col = lax.axis_index("col")
    sub = lax.axis_index("sub")
    even = row % 2 == 0

    every_other = [[first + 2 * i for i in range(n_row // 2)] for first in range(2)]
    strip = lax.all_gather(
        basis_vectors, "row", axis=0, tiled=True, axis_index_groups=every_other
    )

    mate = swapped(basis_vectors, "row")
    pair_t = jnp.concatenate([basis_vectors, mate], axis=0).T
    pair_t = jnp.broadcast_to(pair_t[None], (n_col * lax.axis_size("sub"), *pair_t.shape))

    blocks = [matrix[:, i * block : (i + 1) * block] for i in range(width // block)]
    keep = jnp.concatenate(
        [jnp.where(even, a, b) for a, b in zip(blocks[::2], blocks[1::2])], axis=1
    )
    give = jnp.concatenate(
        [jnp.where(even, b, a) for a, b in zip(blocks[::2], blocks[1::2])], axis=1
    )
    basis_t = lax.all_to_all(pair_t, ("col", "sub"), 0, 0, tiled=True).reshape(-1, 2 * block)
    received = swapped(give, "row")
    own = jnp.concatenate([keep, received], axis=0)

    before = shifted(own, "col", 1)
    after = shifted(own, "col", -1)
    across = shifted(own, "col", 2)
    mine = [own, before, after, across]
    theirs = [swapped(piece, "sub") for piece in mine]

    sources = [col, (col - 1) % n_col, (col + 1) % n_col, (col + 2) % n_col]
    starts = jnp.stack([2 * s + sub for s in sources] + [2 * s + 1 - sub for s in sources])
    share = basis_t.shape[0] // n_row
    keep = kept(split_size[0], row, col, sub, share, 2 * basis_vectors.shape[1])
    starts, keep = lax.optimization_barrier((starts.astype(jnp.int32), keep))
    partial = projected(starts, strip, basis_t, mine + theirs, share)

    far = n_row // NEAR
    near_groups = [[NEAR * g + q for q in range(NEAR)] for g in range(far)]
    far_groups = [[NEAR * g + q for g in range(far)] for q in range(NEAR)]
    partial = lax.all_to_all(
        partial, "row", 0, 0, tiled=True, axis_index_groups=near_groups
    ).sum(0)
    proj_block = lax.all_to_all(
        partial, "row", 0, 0, tiled=True, axis_index_groups=far_groups
    ).sum(0)

    child_block = lax.all_gather(proj_block, "sub", axis=1, tiled=True)
    return jnp.where(keep, child_block, jnp.zeros((), jnp.float32))[None]


def solution(mesh):
    placed = (
        P(("groups", "row"), ("col", "sub")),
        P(("groups", "row"), ("col", "sub")),
        P("groups"),
    )
    return jax.shard_map(
        split_projection,
        mesh=mesh,
        in_specs=placed,
        out_specs=P("sub", ("groups", "row"), "col"),
        check_vma=False,
    )
```

```python
import jax
import jax.numpy as jnp
from jax import lax
from jax.experimental import pallas as pl
from jax.experimental.pallas import tpu as pltpu
from jax.sharding import PartitionSpec as P


NEAR = 4
AHEAD = 3


def shifted(array, axis, step):
    size = lax.axis_size(axis)
    return lax.ppermute(array, axis, [(i, (i + step) % size) for i in range(size)])


def swapped(array, axis):
    size = lax.axis_size(axis)
    return lax.ppermute(array, axis, [(i, i ^ 1) for i in range(size)])


def halves(value):
    high = value.astype(jnp.bfloat16)
    low = (value - high.astype(jnp.float32)).astype(jnp.bfloat16)
    return high, low


def dot(left, right):
    return jnp.dot(left, right, preferred_element_type=jnp.float32)


def project_kernel(starts, strip, basis_t, *refs):
    *pieces, out, chunks, tiles, arrived, landed, image = refs
    wide = strip.shape[1]
    span = chunks.shape[1]
    tile = tiles.shape[2]
    per_piece = tiles.shape[1]

    def chunk_copy(n):
        rows = pl.ds(pl.multiple_of(starts[n] * span, span), span)
        return pltpu.make_async_copy(strip.at[rows], chunks.at[n], arrived.at[n])

    def tile_copy(n, t):
        return pltpu.make_async_copy(pieces[n * per_piece + t], tiles.at[n, t], landed.at[n, t])

    def begin(n):
        chunk_copy(n).start()
        for t in range(per_piece):
            tile_copy(n, t).start()

    for n in range(AHEAD):
        begin(n)
    for n in range(chunks.shape[0]):
        if n + AHEAD < chunks.shape[0]:
            begin(n + AHEAD)
        chunk_copy(n).wait()
        high, low = halves(chunks[n])
        right = jnp.concatenate([high, low], axis=1)
        for t in range(per_piece):
            tile_copy(n, t).wait()
            here = slice(t * tile, (t + 1) * tile)
            left_high, left_low = halves(tiles[n, t])
            both = dot(left_high, right)
            value = both[:, :wide] + (both[:, wide:] + dot(left_low, high))
            if n == 0:
                image[here, :] = value
            else:
                image[here, :] += value

    high, low = halves(image[...])
    right = jnp.concatenate([high, low], axis=1)
    near, far, share = out.shape[:3]
    for f in range(far):
        rows = near * share
        left_high, left_low = halves(basis_t[f * rows : (f + 1) * rows, :])
        both = dot(left_high, right)
        proj = both[:, :wide] + (both[:, wide:] + dot(left_low, high))
        for q in range(near):
            out[q, f] = proj[q * share : (q + 1) * share]


def projected(starts, strip, basis_t, pieces, share):
    per_piece = len(pieces[0])
    tile, span = pieces[0][0].shape
    rows = per_piece * tile
    total, wide = basis_t.shape[0], strip.shape[1]
    n_pieces = len(pieces)
    out_shape = (NEAR, total // share // NEAR, share, wide)
    vmem = pl.BlockSpec(memory_space=pltpu.VMEM)
    anywhere = pl.BlockSpec(memory_space=pl.ANY)
    in_hbm = [
        pltpu.with_memory_space_constraint(array, pltpu.HBM)
        for array in (strip, *(part for piece in pieces for part in piece))
    ]
    return pl.pallas_call(
        project_kernel,
        in_specs=[pl.BlockSpec(memory_space=pltpu.SMEM), anywhere, vmem]
        + [anywhere] * (n_pieces * per_piece),
        out_specs=vmem,
        scratch_shapes=[
            pltpu.VMEM((n_pieces, span, wide), jnp.float32),
            pltpu.VMEM((n_pieces, per_piece, tile, span), jnp.float32),
            pltpu.SemaphoreType.DMA((n_pieces,)),
            pltpu.SemaphoreType.DMA((n_pieces, per_piece)),
            pltpu.VMEM((rows, wide), jnp.float32),
        ],
        out_shape=jax.ShapeDtypeStruct(out_shape, jnp.float32),
        compiler_params=pltpu.CompilerParams(vmem_limit_bytes=32 * 2**20),
        cost_estimate=pl.CostEstimate(
            flops=3 * 2 * rows * wide * (strip.shape[0] + total),
            bytes_accessed=4 * (strip.size + basis_t.size + rows * strip.shape[0]),
            transcendentals=0,
        ),
        name="project",
    )(starts, in_hbm[0], basis_t, *in_hbm[1:])


def kept(leading, row, col, sub, height, width):
    row_ids = jnp.arange(height, dtype=jnp.int32) + row * height
    col_ids = jnp.arange(width, dtype=jnp.int32) + col * width
    row_first = row_ids < leading
    col_first = col_ids < leading
    mask_one = row_first[:, None] & col_first[None, :]
    mask_two = jnp.logical_not(row_first)[:, None] & jnp.logical_not(col_first)[None, :]
    return jnp.where(sub == 0, mask_one, mask_two)


def split_projection(matrix, basis_vectors, split_size):
    block, width = matrix.shape
    n_row = lax.axis_size("row")
    n_col = lax.axis_size("col")
    row = lax.axis_index("row")
    col = lax.axis_index("col")
    sub = lax.axis_index("sub")
    even = row % 2 == 0

    every_other = [[first + 2 * i for i in range(n_row // 2)] for first in range(2)]
    strip = lax.all_gather(
        basis_vectors, "row", axis=0, tiled=True, axis_index_groups=every_other
    )

    mate = swapped(basis_vectors, "row")
    pair_t = jnp.concatenate([basis_vectors, mate], axis=0).T
    pair_t = jnp.broadcast_to(pair_t[None], (n_col * lax.axis_size("sub"), *pair_t.shape))

    blocks = [matrix[:, i * block : (i + 1) * block] for i in range(width // block)]
    keep = jnp.concatenate(
        [jnp.where(even, a, b) for a, b in zip(blocks[::2], blocks[1::2])], axis=1
    )
    give = jnp.concatenate(
        [jnp.where(even, b, a) for a, b in zip(blocks[::2], blocks[1::2])], axis=1
    )
    basis_t = lax.all_to_all(pair_t, ("col", "sub"), 0, 0, tiled=True).reshape(-1, 2 * block)
    received = swapped(give, "row")

    mine, theirs = [], []
    for half in (keep, received):
        copies = [half]
        for step in (1, -1, 2):
            copies.append(shifted(half, "col", step))
        mine.append(copies)
        theirs.append([swapped(copy, "sub") for copy in copies])
    pieces = [*zip(*mine), *zip(*theirs)]

    sources = [col, (col - 1) % n_col, (col + 1) % n_col, (col + 2) % n_col]
    starts = jnp.stack([2 * s + sub for s in sources] + [2 * s + 1 - sub for s in sources])
    share = basis_t.shape[0] // n_row
    inside = kept(split_size[0], row, col, sub, share, 2 * basis_vectors.shape[1])
    starts, inside = lax.optimization_barrier((starts.astype(jnp.int32), inside))
    partial = projected(starts, strip, basis_t, pieces, share)

    far = n_row // NEAR
    near_groups = [[NEAR * g + q for q in range(NEAR)] for g in range(far)]
    far_groups = [[NEAR * g + q for g in range(far)] for q in range(NEAR)]
    partial = lax.all_to_all(
        partial, "row", 0, 0, tiled=True, axis_index_groups=near_groups
    ).sum(0)
    proj_block = lax.all_to_all(
        partial, "row", 0, 0, tiled=True, axis_index_groups=far_groups
    ).sum(0)

    child_block = lax.all_gather(proj_block, "sub", axis=1, tiled=True)
    return jnp.where(inside, child_block, jnp.zeros((), jnp.float32))[None]


def solution(mesh):
    placed = (
        P(("groups", "row"), ("col", "sub")),
        P(("groups", "row"), ("col", "sub")),
        P("groups"),
    )
    return jax.shard_map(
        split_projection,
        mesh=mesh,
        in_specs=placed,
        out_specs=P("sub", ("groups", "row"), "col"),
        check_vma=False,
    )
```

```python
import jax
import jax.numpy as jnp
from jax import lax
from jax.experimental import pallas as pl
from jax.experimental.pallas import tpu as pltpu
from jax.sharding import PartitionSpec as P


NEAR = 4
TILE = 256
AHEAD = 3


def shifted(array, axis, step):
    size = lax.axis_size(axis)
    return lax.ppermute(array, axis, [(i, (i + step) % size) for i in range(size)])


def swapped(array, axis):
    size = lax.axis_size(axis)
    return lax.ppermute(array, axis, [(i, i ^ 1) for i in range(size)])


def halves(value):
    high = value.astype(jnp.bfloat16)
    low = (value - high.astype(jnp.float32)).astype(jnp.bfloat16)
    return high, low


def dot(left, right):
    return jnp.dot(left, right, preferred_element_type=jnp.float32)


def project_kernel(starts, strip, basis_mine, basis_theirs, *refs):
    *pieces, out, chunks, tiles, other, arrived, landed, given, image = refs
    wide = strip.shape[1]
    span = chunks.shape[1]
    per_piece = tiles.shape[1] // TILE
    n_pieces = chunks.shape[0]
    n_whole = (n_pieces * per_piece - len(pieces)) // (per_piece - 1)
    core = starts[n_pieces]

    def chunk_copy(n):
        rows = pl.ds(pl.multiple_of(starts[n] * span, span), span)
        return pltpu.make_async_copy(strip.at[rows], chunks.at[n], arrived.at[n])

    def tile_copy(n, t):
        rows = pl.ds(t * TILE, TILE)
        if n < n_whole:
            source = pieces[n].at[rows]
        else:
            source = pieces[n_whole + (n - n_whole) * per_piece + t]
        return pltpu.make_async_copy(source, tiles.at[n, rows], landed.at[n, t])

    def begin(n):
        chunk_copy(n).start()
        for t in range(per_piece):
            tile_copy(n, t).start()

    for n in range(AHEAD):
        begin(n)
    fetch_basis = pltpu.make_async_copy(basis_theirs, other, given)
    for n in range(n_pieces):
        if n + AHEAD < n_pieces:
            begin(n + AHEAD)
        if n + AHEAD == n_pieces:
            fetch_basis.start()
        chunk_copy(n).wait()
        high, low = halves(chunks[n])
        right = jnp.concatenate([high, low], axis=1)
        for t in range(per_piece):
            tile_copy(n, t).wait()
            here = slice(t * TILE, (t + 1) * TILE)
            left_high, left_low = halves(tiles[n, here])
            both = dot(left_high, right)
            value = both[:, :wide] + (both[:, wide:] + dot(left_low, high))
            if n == 0:
                image[here, :] = value
            else:
                image[here, :] += value

    high, low = halves(image[...])
    right = jnp.concatenate([high, low], axis=1)
    fetch_basis.wait()
    near, far, share = out.shape[:3]
    for basis, which in ((basis_mine, core), (other, 1 - core)):
        for f in range(far // 2):
            left_high, left_low = halves(basis[f])
            both = dot(left_high, right)
            proj = both[:, :wide] + (both[:, wide:] + dot(left_low, high))
            for q in range(near):
                out[q, 2 * f + which] = proj[q * share : (q + 1) * share]


def projected(starts, strip, basis, whole, halved, share):
    rows, span = whole[0].shape
    wide = strip.shape[1]
    total = 2 * basis[0].shape[0] * basis[0].shape[1]
    n_pieces = len(whole) + len(halved)
    pieces = [*whole, *(half for pair in halved for half in pair)]
    out_shape = (NEAR, total // share // NEAR, share, wide)
    vmem = pl.BlockSpec(memory_space=pltpu.VMEM)
    anywhere = pl.BlockSpec(memory_space=pl.ANY)
    strip = pltpu.with_memory_space_constraint(strip, pltpu.HBM)
    basis_theirs = pltpu.with_memory_space_constraint(basis[1], pltpu.HBM)
    return pl.pallas_call(
        project_kernel,
        in_specs=[pl.BlockSpec(memory_space=pltpu.SMEM), anywhere, vmem, anywhere]
        + [anywhere] * len(pieces),
        out_specs=vmem,
        scratch_shapes=[
            pltpu.VMEM((n_pieces, span, wide), jnp.float32),
            pltpu.VMEM((n_pieces, rows, span), jnp.float32),
            pltpu.VMEM(basis[1].shape, jnp.float32),
            pltpu.SemaphoreType.DMA((n_pieces,)),
            pltpu.SemaphoreType.DMA((n_pieces, rows // TILE)),
            pltpu.SemaphoreType.DMA(()),
            pltpu.VMEM((rows, wide), jnp.float32),
        ],
        out_shape=jax.ShapeDtypeStruct(out_shape, jnp.float32),
        compiler_params=pltpu.CompilerParams(vmem_limit_bytes=32 * 2**20),
        cost_estimate=pl.CostEstimate(
            flops=3 * 2 * rows * wide * (strip.shape[0] + total),
            bytes_accessed=4 * (strip.size + 2 * basis[0].size + rows * strip.shape[0]),
            transcendentals=0,
        ),
        name="project",
    )(starts, strip, basis[0], basis_theirs, *pieces)


def kept(leading, row, col, sub, height, width):
    row_ids = jnp.arange(height, dtype=jnp.int32) + row * height
    col_ids = jnp.arange(width, dtype=jnp.int32) + col * width
    row_first = row_ids < leading
    col_first = col_ids < leading
    mask_one = row_first[:, None] & col_first[None, :]
    mask_two = jnp.logical_not(row_first)[:, None] & jnp.logical_not(col_first)[None, :]
    return jnp.where(sub == 0, mask_one, mask_two)


def split_projection(matrix, basis_vectors, split_size):
    block, width = matrix.shape
    n_row = lax.axis_size("row")
    n_col = lax.axis_size("col")
    row = lax.axis_index("row")
    col = lax.axis_index("col")
    sub = lax.axis_index("sub")
    even = row % 2 == 0

    every_other = [[first + 2 * i for i in range(n_row // 2)] for first in range(2)]
    strip = lax.all_gather(
        basis_vectors, "row", axis=0, tiled=True, axis_index_groups=every_other
    )

    mate = swapped(basis_vectors, "row")
    pair_t = jnp.concatenate([basis_vectors, mate], axis=0).T
    pair_t = jnp.broadcast_to(pair_t[None], (n_col, *pair_t.shape))

    blocks = [matrix[:, i * block : (i + 1) * block] for i in range(width // block)]
    keep = jnp.concatenate(
        [jnp.where(even, a, b) for a, b in zip(blocks[::2], blocks[1::2])], axis=1
    )
    give = jnp.concatenate(
        [jnp.where(even, b, a) for a, b in zip(blocks[::2], blocks[1::2])], axis=1
    )
    basis_mine = lax.all_to_all(pair_t, "col", 0, 0, tiled=True)
    received = swapped(give, "row")
    own = jnp.concatenate([keep, received], axis=0)

    before = shifted(own, "col", 1)
    after = shifted(own, "col", -1)
    across = (shifted(before[:block], "col", 1), shifted(after[block:], "col", -1))
    mine = [own, before, after]
    theirs = [swapped(piece, "sub") for piece in mine]
    across_other = tuple(swapped(piece, "sub") for piece in across)
    basis = (basis_mine, swapped(basis_mine, "sub"))

    sources = [col, (col - 1) % n_col, (col + 1) % n_col]
    opposite = (col + 2) % n_col
    starts = jnp.stack(
        [2 * s + sub for s in sources]
        + [2 * s + 1 - sub for s in sources]
        + [2 * opposite + sub, 2 * opposite + 1 - sub, sub]
    )
    share = 2 * n_col * basis_vectors.shape[1] // n_row
    keep = kept(split_size[0], row, col, sub, share, 2 * basis_vectors.shape[1])
    starts, keep = lax.optimization_barrier((starts.astype(jnp.int32), keep))
    partial = projected(starts, strip, basis, mine + theirs, (across, across_other), share)

    far = n_row // NEAR
    near_groups = [[NEAR * g + q for q in range(NEAR)] for g in range(far)]
    far_groups = [[NEAR * g + q for g in range(far)] for q in range(NEAR)]
    partial = lax.all_to_all(
        partial, "row", 0, 0, tiled=True, axis_index_groups=near_groups
    ).sum(0)
    proj_block = lax.all_to_all(
        partial, "row", 0, 0, tiled=True, axis_index_groups=far_groups
    ).sum(0)

    child_block = lax.all_gather(proj_block, "sub", axis=1, tiled=True)
    return jnp.where(keep, child_block, jnp.zeros((), jnp.float32))[None]


def solution(mesh):
    placed = (
        P(("groups", "row"), ("col", "sub")),
        P(("groups", "row"), ("col", "sub")),
        P("groups"),
    )
    return jax.shard_map(
        split_projection,
        mesh=mesh,
        in_specs=placed,
        out_specs=P("sub", ("groups", "row"), "col"),
        check_vma=False,
    )
```

```python
import jax
import jax.numpy as jnp
from jax import lax
from jax.experimental import pallas as pl
from jax.experimental.pallas import tpu as pltpu
from jax.sharding import PartitionSpec as P


NEAR = 4
TILE = 256
AHEAD = 3


def shifted(array, axis, step):
    size = lax.axis_size(axis)
    return lax.ppermute(array, axis, [(i, (i + step) % size) for i in range(size)])


def swapped(array, axis):
    size = lax.axis_size(axis)
    return lax.ppermute(array, axis, [(i, i ^ 1) for i in range(size)])


def halves(value):
    high = value.astype(jnp.bfloat16)
    low = (value - high.astype(jnp.float32)).astype(jnp.bfloat16)
    return high, low


def dot(left, right):
    return jnp.dot(left, right, preferred_element_type=jnp.float32)


def split_kernel(piece, out):
    width = piece.shape[1]
    high, low = halves(piece[...])
    out[:, :width] = high
    out[:, width:] = low


def split(piece):
    rows, width = piece.shape
    tile = TILE // 2
    return pl.pallas_call(
        split_kernel,
        grid=(rows // tile,),
        in_specs=[pl.BlockSpec((tile, width), lambda i: (i, 0))],
        out_specs=pl.BlockSpec((tile, 2 * width), lambda i: (i, 0)),
        out_shape=pltpu.HBM((rows, 2 * width), jnp.bfloat16),
        compiler_params=pltpu.CompilerParams(
            dimension_semantics=("arbitrary",), vmem_limit_bytes=8 * 2**20
        ),
        cost_estimate=pl.CostEstimate(
            flops=3 * piece.size, bytes_accessed=8 * piece.size, transcendentals=0
        ),
        name="split",
    )(piece)


def project_kernel(starts, strip, basis_mine, basis_theirs, *refs):
    *pieces, out, chunks, tiles, other, arrived, landed, given, image = refs
    wide = strip.shape[1]
    span = chunks.shape[1]
    per_piece = tiles.shape[1] // TILE
    n_pieces = chunks.shape[0]
    n_whole = (n_pieces * per_piece - len(pieces)) // (per_piece - 1)
    core = starts[n_pieces]

    def chunk_copy(n):
        rows = pl.ds(pl.multiple_of(starts[n] * span, span), span)
        return pltpu.make_async_copy(strip.at[rows], chunks.at[n], arrived.at[n])

    def tile_copy(n, t):
        rows = pl.ds(t * TILE, TILE)
        if n < n_whole:
            source = pieces[n].at[rows]
        else:
            source = pieces[n_whole + (n - n_whole) * per_piece + t]
        return pltpu.make_async_copy(source, tiles.at[n, rows], landed.at[n, t])

    def begin(n):
        chunk_copy(n).start()
        for t in range(per_piece):
            tile_copy(n, t).start()

    for n in range(AHEAD):
        begin(n)
    fetch_basis = pltpu.make_async_copy(basis_theirs, other, given)
    for n in range(n_pieces):
        if n + AHEAD < n_pieces:
            begin(n + AHEAD)
        if n + AHEAD == n_pieces:
            fetch_basis.start()
        chunk_copy(n).wait()
        high, low = halves(chunks[n])
        right = jnp.concatenate([high, low], axis=1)
        for t in range(per_piece):
            tile_copy(n, t).wait()
            here = slice(t * TILE, (t + 1) * TILE)
            both = dot(tiles[n, here, :span], right)
            value = both[:, :wide] + (both[:, wide:] + dot(tiles[n, here, span:], high))
            if n == 0:
                image[here, :] = value
            else:
                image[here, :] += value

    high, low = halves(image[...])
    right = jnp.concatenate([high, low], axis=1)
    fetch_basis.wait()
    near, far, share = out.shape[:3]
    for basis, which in ((basis_mine, core), (other, 1 - core)):
        for f in range(far // 2):
            left_high, left_low = halves(basis[f])
            both = dot(left_high, right)
            proj = both[:, :wide] + (both[:, wide:] + dot(left_low, high))
            for q in range(near):
                out[q, 2 * f + which] = proj[q * share : (q + 1) * share]


def projected(starts, strip, basis, whole, halved, share):
    rows, span = whole[0].shape[0], whole[0].shape[1] // 2
    wide = strip.shape[1]
    total = 2 * basis[0].shape[0] * basis[0].shape[1]
    n_pieces = len(whole) + len(halved)
    pieces = [
        pltpu.with_memory_space_constraint(piece, pltpu.HBM)
        for piece in (*whole, *(half for pair in halved for half in pair))
    ]
    out_shape = (NEAR, total // share // NEAR, share, wide)
    vmem = pl.BlockSpec(memory_space=pltpu.VMEM)
    anywhere = pl.BlockSpec(memory_space=pl.ANY)
    strip = pltpu.with_memory_space_constraint(strip, pltpu.HBM)
    basis_theirs = pltpu.with_memory_space_constraint(basis[1], pltpu.HBM)
    return pl.pallas_call(
        project_kernel,
        in_specs=[pl.BlockSpec(memory_space=pltpu.SMEM), anywhere, vmem, anywhere]
        + [anywhere] * len(pieces),
        out_specs=vmem,
        scratch_shapes=[
            pltpu.VMEM((n_pieces, span, wide), jnp.float32),
            pltpu.VMEM((n_pieces, rows, 2 * span), jnp.bfloat16),
            pltpu.VMEM(basis[1].shape, jnp.float32),
            pltpu.SemaphoreType.DMA((n_pieces,)),
            pltpu.SemaphoreType.DMA((n_pieces, rows // TILE)),
            pltpu.SemaphoreType.DMA(()),
            pltpu.VMEM((rows, wide), jnp.float32),
        ],
        out_shape=jax.ShapeDtypeStruct(out_shape, jnp.float32),
        compiler_params=pltpu.CompilerParams(vmem_limit_bytes=32 * 2**20),
        cost_estimate=pl.CostEstimate(
            flops=3 * 2 * rows * wide * (strip.shape[0] + total),
            bytes_accessed=4 * (strip.size + 2 * basis[0].size + rows * strip.shape[0]),
            transcendentals=0,
        ),
        name="project",
    )(starts, strip, basis[0], basis_theirs, *pieces)


def kept(leading, row, col, sub, height, width):
    row_ids = jnp.arange(height, dtype=jnp.int32) + row * height
    col_ids = jnp.arange(width, dtype=jnp.int32) + col * width
    row_first = row_ids < leading
    col_first = col_ids < leading
    mask_one = row_first[:, None] & col_first[None, :]
    mask_two = jnp.logical_not(row_first)[:, None] & jnp.logical_not(col_first)[None, :]
    return jnp.where(sub == 0, mask_one, mask_two)


def split_projection(matrix, basis_vectors, split_size):
    block, width = matrix.shape
    n_row = lax.axis_size("row")
    n_col = lax.axis_size("col")
    row = lax.axis_index("row")
    col = lax.axis_index("col")
    sub = lax.axis_index("sub")
    even = row % 2 == 0

    every_other = [[first + 2 * i for i in range(n_row // 2)] for first in range(2)]
    strip = lax.all_gather(
        basis_vectors, "row", axis=0, tiled=True, axis_index_groups=every_other
    )

    mate = swapped(basis_vectors, "row")
    pair_t = jnp.concatenate([basis_vectors, mate], axis=0).T
    pair_t = jnp.broadcast_to(pair_t[None], (n_col, *pair_t.shape))

    blocks = [matrix[:, i * block : (i + 1) * block] for i in range(width // block)]
    keep = jnp.concatenate(
        [jnp.where(even, a, b) for a, b in zip(blocks[::2], blocks[1::2])], axis=1
    )
    give = jnp.concatenate(
        [jnp.where(even, b, a) for a, b in zip(blocks[::2], blocks[1::2])], axis=1
    )
    basis_mine = lax.all_to_all(pair_t, "col", 0, 0, tiled=True)
    received = swapped(give, "row")
    own = jnp.concatenate([keep, received], axis=0)

    before = shifted(own, "col", 1)
    after = shifted(own, "col", -1)
    across = (shifted(before[:block], "col", 1), shifted(after[block:], "col", -1))
    mine = [own, before, after]
    theirs = [swapped(piece, "sub") for piece in mine]
    across_other = tuple(swapped(piece, "sub") for piece in across)
    basis = (basis_mine, swapped(basis_mine, "sub"))

    sources = [col, (col - 1) % n_col, (col + 1) % n_col]
    opposite = (col + 2) % n_col
    starts = jnp.stack(
        [2 * s + sub for s in sources]
        + [2 * s + 1 - sub for s in sources]
        + [2 * opposite + sub, 2 * opposite + 1 - sub, sub]
    )
    share = 2 * n_col * basis_vectors.shape[1] // n_row
    keep = kept(split_size[0], row, col, sub, share, 2 * basis_vectors.shape[1])
    starts, keep = lax.optimization_barrier((starts.astype(jnp.int32), keep))
    whole = [split(piece) for piece in mine + theirs]
    halved = [tuple(split(half) for half in pair) for pair in (across, across_other)]
    partial = projected(starts, strip, basis, whole, halved, share)

    far = n_row // NEAR
    near_groups = [[NEAR * g + q for q in range(NEAR)] for g in range(far)]
    far_groups = [[NEAR * g + q for g in range(far)] for q in range(NEAR)]
    partial = lax.all_to_all(
        partial, "row", 0, 0, tiled=True, axis_index_groups=near_groups
    ).sum(0)
    proj_block = lax.all_to_all(
        partial, "row", 0, 0, tiled=True, axis_index_groups=far_groups
    ).sum(0)

    child_block = lax.all_gather(proj_block, "sub", axis=1, tiled=True)
    return jnp.where(keep, child_block, jnp.zeros((), jnp.float32))[None]


def solution(mesh):
    placed = (
        P(("groups", "row"), ("col", "sub")),
        P(("groups", "row"), ("col", "sub")),
        P("groups"),
    )
    return jax.shard_map(
        split_projection,
        mesh=mesh,
        in_specs=placed,
        out_specs=P("sub", ("groups", "row"), "col"),
        check_vma=False,
    )
```

```python
import jax
import jax.numpy as jnp
from jax import lax
from jax.experimental import pallas as pl
from jax.experimental.pallas import tpu as pltpu
from jax.sharding import PartitionSpec as P


NEAR = 4
TILE = 256
AHEAD = 5


def shifted(array, axis, step):
    size = lax.axis_size(axis)
    return lax.ppermute(array, axis, [(i, (i + step) % size) for i in range(size)])


def swapped(array, axis):
    size = lax.axis_size(axis)
    return lax.ppermute(array, axis, [(i, i ^ 1) for i in range(size)])


def halves(value):
    high = value.astype(jnp.bfloat16)
    low = (value - high.astype(jnp.float32)).astype(jnp.bfloat16)
    return high, low


def dot(left, right):
    return jnp.dot(left, right, preferred_element_type=jnp.float32)


def dot_nt(left, right):
    return lax.dot_general(
        left, right, (((1,), (1,)), ((), ())), preferred_element_type=jnp.float32
    )


def project_kernel(starts, strip, basis_mine, basis_theirs, *refs):
    *pieces, out, chunks, tiles, other, arrived, landed, given, image_t = refs
    wide = strip.shape[1]
    span = chunks.shape[1]
    per_piece = tiles.shape[1] // TILE
    n_pieces = chunks.shape[0]
    n_whole = (n_pieces * per_piece - len(pieces)) // (per_piece - 1)
    core = starts[n_pieces]

    def chunk_copy(n):
        rows = pl.ds(pl.multiple_of(starts[n] * span, span), span)
        return pltpu.make_async_copy(strip.at[rows], chunks.at[n], arrived.at[n])

    def tile_copy(n, t):
        rows = pl.ds(t * TILE, TILE)
        if n < n_whole:
            source = pieces[n].at[rows]
        else:
            source = pieces[n_whole + (n - n_whole) * per_piece + t]
        return pltpu.make_async_copy(source, tiles.at[n, rows], landed.at[n, t])

    def start_copies(n):
        chunk_copy(n).start(priority=1)
        for t in range(per_piece):
            tile_copy(n, t).start()

    for n in range(AHEAD):
        start_copies(n)
    fetch_basis = pltpu.make_async_copy(basis_theirs, other, given)
    for n in range(n_pieces):
        if n + AHEAD < n_pieces:
            start_copies(n + AHEAD)
        if n + AHEAD == n_pieces:
            fetch_basis.start()
        chunk_copy(n).wait()
        high, low = halves(chunks[n])
        for t in range(per_piece):
            tile_copy(n, t).wait()
        piece_high, piece_low = halves(tiles[n])
        stacked = jnp.concatenate([high.T, low.T], axis=0)
        both = dot_nt(stacked, piece_high)
        value = both[:wide] + (both[wide:] + dot_nt(high.T, piece_low))
        if n == 0:
            image_t[...] = value
        else:
            image_t[...] += value

    high, low = halves(image_t[...].T)
    right = jnp.concatenate([high, low], axis=1)
    fetch_basis.wait()
    near, far, share = out.shape[:3]
    for basis, which in ((basis_mine, core), (other, 1 - core)):
        for f in range(far // 2):
            left_high, left_low = halves(basis[f])
            both = dot(left_high, right)
            proj = both[:, :wide] + (both[:, wide:] + dot(left_low, high))
            for q in range(near):
                out[q, 2 * f + which] = proj[q * share : (q + 1) * share]


def projected(starts, strip, basis, whole, halved, share):
    rows, span = whole[0].shape
    wide = strip.shape[1]
    total = 2 * basis[0].shape[0] * basis[0].shape[1]
    n_pieces = len(whole) + len(halved)
    pieces = [*whole, *(half for pair in halved for half in pair)]
    out_shape = (NEAR, total // share // NEAR, share, wide)
    vmem = pl.BlockSpec(memory_space=pltpu.VMEM)
    anywhere = pl.BlockSpec(memory_space=pl.ANY)
    strip = pltpu.with_memory_space_constraint(strip, pltpu.HBM)
    basis_theirs = pltpu.with_memory_space_constraint(basis[1], pltpu.HBM)
    return pl.pallas_call(
        project_kernel,
        in_specs=[pl.BlockSpec(memory_space=pltpu.SMEM), anywhere, vmem, anywhere]
        + [anywhere] * len(pieces),
        out_specs=vmem,
        scratch_shapes=[
            pltpu.VMEM((n_pieces, span, wide), jnp.float32),
            pltpu.VMEM((n_pieces, rows, span), jnp.float32),
            pltpu.VMEM(basis[1].shape, jnp.float32),
            pltpu.SemaphoreType.DMA((n_pieces,)),
            pltpu.SemaphoreType.DMA((n_pieces, rows // TILE)),
            pltpu.SemaphoreType.DMA(()),
            pltpu.VMEM((wide, rows), jnp.float32),
        ],
        out_shape=jax.ShapeDtypeStruct(out_shape, jnp.float32),
        compiler_params=pltpu.CompilerParams(vmem_limit_bytes=32 * 2**20),
        cost_estimate=pl.CostEstimate(
            flops=3 * 2 * rows * wide * (strip.shape[0] + total),
            bytes_accessed=4 * (strip.size + 2 * basis[0].size + rows * strip.shape[0]),
            transcendentals=0,
        ),
        name="project",
    )(starts, strip, basis[0], basis_theirs, *pieces)


def kept(leading, row, col, sub, height, width):
    row_ids = jnp.arange(height, dtype=jnp.int32) + row * height
    col_ids = jnp.arange(width, dtype=jnp.int32) + col * width
    row_first = row_ids < leading
    col_first = col_ids < leading
    mask_one = row_first[:, None] & col_first[None, :]
    mask_two = jnp.logical_not(row_first)[:, None] & jnp.logical_not(col_first)[None, :]
    return jnp.where(sub == 0, mask_one, mask_two)


def split_projection(matrix, basis_vectors, split_size):
    block, width = matrix.shape
    n_row = lax.axis_size("row")
    n_col = lax.axis_size("col")
    row = lax.axis_index("row")
    col = lax.axis_index("col")
    sub = lax.axis_index("sub")
    even = row % 2 == 0

    every_other = [[first + 2 * i for i in range(n_row // 2)] for first in range(2)]
    strip = lax.all_gather(
        basis_vectors, "row", axis=0, tiled=True, axis_index_groups=every_other
    )

    mate = swapped(basis_vectors, "row")
    pair_t = jnp.concatenate([basis_vectors, mate], axis=0).T
    pair_t = jnp.broadcast_to(pair_t[None], (n_col, *pair_t.shape))

    blocks = [matrix[:, i * block : (i + 1) * block] for i in range(width // block)]
    keep = jnp.concatenate(
        [jnp.where(even, a, b) for a, b in zip(blocks[::2], blocks[1::2])], axis=1
    )
    give = jnp.concatenate(
        [jnp.where(even, b, a) for a, b in zip(blocks[::2], blocks[1::2])], axis=1
    )
    basis_mine = lax.all_to_all(pair_t, "col", 0, 0, tiled=True)
    received = swapped(give, "row")
    own = jnp.concatenate([keep, received], axis=0)

    before = shifted(own, "col", 1)
    after = shifted(own, "col", -1)
    across = (shifted(before[:block], "col", 1), shifted(after[block:], "col", -1))
    mine = [own, before, after]
    theirs = [swapped(piece, "sub") for piece in mine]
    across_other = tuple(swapped(piece, "sub") for piece in across)
    basis = (basis_mine, swapped(basis_mine, "sub"))

    sources = [col, (col - 1) % n_col, (col + 1) % n_col]
    opposite = (col + 2) % n_col
    starts = jnp.stack(
        [2 * s + sub for s in sources]
        + [2 * s + 1 - sub for s in sources]
        + [2 * opposite + sub, 2 * opposite + 1 - sub, sub]
    )
    share = 2 * n_col * basis_vectors.shape[1] // n_row
    keep = kept(split_size[0], row, col, sub, share, 2 * basis_vectors.shape[1])
    starts, keep = lax.optimization_barrier((starts.astype(jnp.int32), keep))
    partial = projected(starts, strip, basis, mine + theirs, (across, across_other), share)

    far = n_row // NEAR
    near_groups = [[NEAR * g + q for q in range(NEAR)] for g in range(far)]
    far_groups = [[NEAR * g + q for g in range(far)] for q in range(NEAR)]
    partial = lax.all_to_all(
        partial, "row", 0, 0, tiled=True, axis_index_groups=near_groups
    ).sum(0)
    proj_block = lax.all_to_all(
        partial, "row", 0, 0, tiled=True, axis_index_groups=far_groups
    ).sum(0)

    child_block = lax.all_gather(proj_block, "sub", axis=1, tiled=True)
    return jnp.where(keep, child_block, jnp.zeros((), jnp.float32))[None]


def solution(mesh):
    placed = (
        P(("groups", "row"), ("col", "sub")),
        P(("groups", "row"), ("col", "sub")),
        P("groups"),
    )
    return jax.shard_map(
        split_projection,
        mesh=mesh,
        in_specs=placed,
        out_specs=P("sub", ("groups", "row"), "col"),
        check_vma=False,
    )
```
